256 devices in a mesh: north: 64 (over z_lo, y, x, core), east: 4 (over z_hi).
Axes of the slice: x: 4, y: 4, z: 8 (z_hi: 4, z_lo: 2; z = z_hi * 2 + z_lo), core: 2. Of those that a mesh axis runs over, the one named last changes fastest.
Arguments:
- right_side: float32 [4096, 256, 256], P('north', 'east'), may hold values from -6 to 6
- first_guess: float32 [4096, 256, 256], P('north', 'east'), may hold values from -6 to 6
- mass_term: float32 [4096, 256, 256], P('north', 'east'), may hold values from 0.1 to 0.9
Outputs:
- corrected: float32 [4096, 256, 256], P('north', 'east')
- remaining: float32 [4096, 256, 256], P('north', 'east')
The draws below stay inside these ranges and needn't reach their ends.
All inputs are finite; a program needn't handle non-finite values.
Results may differ from the reference program's by a relative error of at most 0.000032.
Values sent between devices are 32-bit elements; how exact they have to be, the bound alone decides.
No kernel may reach another device: no remote copies, remote signals or barrier semaphores. Data moves between devices by JAX's collectives and lax.ppermute only.
A program may use at most 128 MiB of HBM per device.

```python
import jax
import jax.numpy as jnp
from jax import lax

CASES = 256
RATIO = 2
BEFORE = 2
AFTER = 2
INNER = 7
GRID_Y = 4096
GRID_X = 256


def steps_of(key, dims, split, smallest, largest):
    loudness, own = 1.0, jax.random.fold_in(key, 6)
    for axis_at, shards_of in split:
        draws = jnp.exp(jax.random.uniform(jax.random.fold_in(own, axis_at), (shards_of,), jnp.float32, smallest / len(split), largest / len(split)))
        loudness = loudness * jnp.repeat(draws, dims[axis_at] // shards_of).reshape([-1 if axis == axis_at else 1 for axis in range(len(dims))])
    return loudness


def gaussian(stream_key, extent, width, bound, pieces=(), dtype=jnp.bfloat16):
    entries = width * jax.random.normal(stream_key, extent, jnp.float32)
    if pieces:
        entries = entries * steps_of(stream_key, extent, pieces, -0.22, 0.18)
    return jnp.clip(entries, -bound, bound).astype(dtype)


def setup_inputs(seed: int = 0) -> dict:
    key_of = jax.random.split(jax.random.key(seed), 4)
    right_side = gaussian(key_of[0], (GRID_Y, GRID_X, CASES), 1.0, 6.0, ((0, 64), (1, 4)), jnp.float32)
    first_guess = gaussian(key_of[1], (GRID_Y, GRID_X, CASES), 1.0, 6.0, ((0, 64), (1, 4)), jnp.float32)
    mass_term = jnp.clip(0.1 + 0.79999997 * jax.random.uniform(key_of[2], (GRID_Y, GRID_X, CASES), jnp.float32) ** steps_of(key_of[2], (GRID_Y, GRID_X, CASES), ((0, 64), (1, 4)), -0.2, 0.2), 0.1, 0.9)
    return dict(right_side=right_side, first_guess=first_guess, mass_term=mass_term)


def cross_sum(padded):
    inner_y, inner_x = padded.shape[0] - 2, padded.shape[1] - 2
    middle_rows = lax.slice_in_dim(padded, 1, 1 + inner_y, axis=0)
    middle_columns = lax.slice_in_dim(padded, 1, 1 + inner_x, axis=1)
    return (lax.slice_in_dim(middle_columns, 0, inner_y, axis=0) + lax.slice_in_dim(middle_columns, 2, 2 + inner_y, axis=0)
            + lax.slice_in_dim(middle_rows, 0, inner_x, axis=1) + lax.slice_in_dim(middle_rows, 2, 2 + inner_x, axis=1))


def smooth_step(padded, values, load, mass_here):
    return values + 0.8 * (load + cross_sum(padded) - (4.0 + mass_here) * values) / (4.0 + mass_here)


def block_means(values):
    cut = values.reshape(values.shape[0] // RATIO, RATIO, values.shape[1] // RATIO, RATIO, values.shape[2])
    return jnp.mean(cut, axis=(1, 3))


def spread_blocks(values):
    return jnp.repeat(jnp.repeat(values, RATIO, axis=0), RATIO, axis=1)


def reference(right_side, first_guess, mass_term):
    values = first_guess
    for sweep in range(BEFORE):
        values = smooth_step(jnp.pad(values, ((1, 1), (1, 1), (0, 0)), mode="wrap"), values, right_side, mass_term)
    defect = right_side + cross_sum(jnp.pad(values, ((1, 1), (1, 1), (0, 0)), mode="wrap")) - (4.0 + mass_term) * values
    coarse_load, coarse_mass = block_means(defect) * RATIO, block_means(mass_term) * RATIO
    coarse_values = jnp.zeros_like(coarse_load)
    for sweep in range(INNER):
        coarse_values = smooth_step(jnp.pad(coarse_values, ((1, 1), (1, 1), (0, 0)), mode="wrap"), coarse_values, coarse_load, coarse_mass)
    values = values + spread_blocks(coarse_values)
    for sweep in range(AFTER):
        values = smooth_step(jnp.pad(values, ((1, 1), (1, 1), (0, 0)), mode="wrap"), values, right_side, mass_term)
    corrected = values
    remaining = right_side + cross_sum(jnp.pad(corrected, ((1, 1), (1, 1), (0, 0)), mode="wrap")) - (4.0 + mass_term) * corrected
    return corrected, remaining
```

```python
import jax
import jax.numpy as jnp
from jax import lax
from jax.experimental import pallas as pl
from jax.experimental.pallas import tpu as pltpu
from jax.sharding import PartitionSpec as P

NY, NX, NC = 64, 64, 256
HALVES = 2
LANES = 128
DEEP = 3
LEFT = 16
FY, FX = NY + 2 * DEEP, NX + 2 * LEFT
CY, CX = NY // 2, NX // 2
WIDE = 6
TOP = 8
GY, GX = CY + 20, CX + 2 * LEFT
BLOCK = 4

VMEM = pltpu.VMEM
F32 = jnp.float32
IN_VMEM = pl.BlockSpec(memory_space=VMEM)
IN_HBM = pl.BlockSpec(memory_space=pltpu.HBM)


def corner_cells(arrays):
    cells = []
    for k, (at, deep) in enumerate(arrays):
        for side in range(2):
            for dy in range(1, deep):
                cells.append((side, at + (deep - dy if side == 0 else dy - 1), deep - dy, k, dy))
    return cells


INPUTS = ((0, 3), (3, 2), (5, 2))
COARSE = ((0, WIDE), (WIDE, WIDE))
VALUES = ((0, 3),)


def half(c):
    return pl.ds(c * LANES, LANES)


def shape(*dims):
    return jax.ShapeDtypeStruct(dims, F32)


def exchange(low, high, axis):
    size = lax.axis_size(axis)
    up = [(i, (i + 1) % size) for i in range(size)]
    down = [(b, a) for a, b in up]
    return lax.ppermute(high, axis, up), lax.ppermute(low, axis, down)


def pack_kernel(cells, width, n_lo, n_hi, down, up):
    at = 0
    for side, row, n, _, _ in cells:
        src = (n_lo, n_hi)[side]
        down[pl.ds(at, n), :] = src[row, pl.ds(0, n), :]
        up[pl.ds(at, n), :] = src[row, pl.ds(width - n, n), :]
        at += n


def pack(cells, n_lo, n_hi):
    size = -(-sum(c[2] for c in cells) // 8) * 8
    return pl.pallas_call(
        lambda *refs: pack_kernel(cells, n_lo.shape[1], *refs),
        out_shape=(shape(size, NC),) * 2,
        in_specs=[IN_VMEM] * 2,
        out_specs=(IN_VMEM,) * 2,
        compiler_params=pltpu.CompilerParams(vmem_limit_bytes=8 * 2**20),
        name="pack",
    )(n_lo, n_hi)


def halos(arrays, east_low, east_high, north_low, north_high):
    e_lo, e_hi = exchange(east_low, east_high, "east")
    n_lo, n_hi = exchange(north_low, north_high, "north")
    down, up = pack(corner_cells(arrays), n_lo, n_hi)
    c_lo, c_hi = exchange(down, up, "east")
    return e_lo, e_hi, n_lo, n_hi, c_lo, c_hi


def edges_kernel(u_ref, f_ref, m_ref, el_ref, eh_ref, nl_ref, nh_ref, tiles, sems, row_sems):
    arrays = ((u_ref, 3, 0), (f_ref, 2, 3), (m_ref, 2, 5))
    copies = []
    rows = []
    for k, (ref, deep, at) in enumerate(arrays):
        for side in range(2):
            for c in range(HALVES):
                cp = pltpu.make_async_copy(
                    ref.at[:, pl.ds(side * (NX - 8), 8), half(c)],
                    tiles.at[k, side, c],
                    sems.at[k, side, c],
                )
                cp.start()
                copies.append((cp, k, side, c, deep, at))
            out = (nl_ref, nh_ref)[side]
            start = 0 if side == 0 else NY - deep
            cp = pltpu.make_async_copy(
                ref.at[pl.ds(start, deep)], out.at[pl.ds(at, deep)], row_sems.at[k, side]
            )
            cp.start()
            rows.append(cp)
    for cp, k, side, c, deep, at in copies:
        cp.wait()
        flat = tiles.at[k, side, c].reshape(NY * 8, LANES)
        out = (el_ref, eh_ref)[side]
        first = 0 if side == 0 else 8 - deep
        for d in range(deep):
            out[at + d, :, half(c)] = flat[pl.ds(first + d, NY, stride=8), :]
    for cp in rows:
        cp.wait()


def edges(u, f, m):
    return pl.pallas_call(
        edges_kernel,
        out_shape=(shape(7, NY, NC),) * 4,
        in_specs=[IN_HBM] * 3,
        out_specs=(IN_VMEM,) * 4,
        scratch_shapes=[
            VMEM((3, 2, HALVES, NY, 8, LANES), F32),
            pltpu.SemaphoreType.DMA((3, 2, HALVES)),
            pltpu.SemaphoreType.DMA((3, 2)),
        ],
        compiler_params=pltpu.CompilerParams(vmem_limit_bytes=16 * 2**20),
        name="edges",
    )(u, f, m)


def place_halo(dst, h, sizes, at, deep, array, cells, e_lo, e_hi, n_lo, n_hi, c_lo, c_hi):
    top, ny, nx, pitch = sizes
    cols = pl.ds(LEFT, nx)
    dst[pl.ds(top - deep, deep), cols, :] = n_lo[pl.ds(at, deep), :, h]
    dst[pl.ds(top + ny, deep), cols, :] = n_hi[pl.ds(at, deep), :, h]
    where = 0
    for side, _, n, k, dy in cells:
        if k == array:
            row = top - dy if side == 0 else top + ny + dy - 1
            dst[row, pl.ds(LEFT - n, n), :] = c_lo[pl.ds(where, n), h]
            dst[row, pl.ds(LEFT + nx, n), :] = c_hi[pl.ds(where, n), h]
        where += n
    flat = dst.reshape(dst.shape[0] * pitch, LANES)
    for d in range(deep):
        flat[pl.ds(top * pitch + LEFT - deep + d, ny, stride=pitch), :] = e_lo[at + d, :, h]
        flat[pl.ds(top * pitch + LEFT + nx + d, ny, stride=pitch), :] = e_hi[at + d, :, h]


FINE = (DEEP, NY, NX, FX)


def stencil(src, r, col, count, height):
    last = lax.broadcasted_iota(jnp.int32, (8, LANES), 0) == 7
    cache = {}

    def tile(k, t):
        if (k, t) not in cache:
            cache[k, t] = src[r + k, pl.ds(col + 8 * t, 8), :]
        return cache[k, t]

    turn = [pltpu.roll(tile(k, 0), 7, 0) for k in range(height)]
    for t in range(count):
        for k in range(height):
            following = pltpu.roll(tile(k, t + 1), 7, 0)
            right = jnp.where(last, following, turn[k])
            turn[k] = following
            left = src[r + k, pl.ds(col + 8 * t - 1, 8), :]
            yield k, t, tile(k, t), (tile(k - 1, t) + tile(k + 1, t)) + (left + right)


def sweep_rows(src, dst, load, weight, start, rows, col, count, mass=None):
    def block(i, carry):
        r = start + BLOCK * i
        for k, t, mid, s in stencil(src, r, col, count, BLOCK):
            at = pl.ds(col + 8 * t, 8)
            if mass is None:
                w = weight[r + k, at, :]
            else:
                w = 0.8 / (4.0 + mass[r + k, at, :])
                weight[r + k, at, :] = w
            dst[r + k, at, :] = 0.2 * mid + w * (s + load[r + k, at, :])
        return carry

    lax.fori_loop(0, rows // BLOCK, block, 0)


def two_sweeps(us, vs, fs, ms, ws):
    args = (1, NY + 4, LEFT - 8, NX // 8 + 2)
    sweep_rows(us, vs, fs, ws, *args, mass=ms)
    sweep_rows(vs, us, fs, ws, *args)


def fetch(refs, dsts, sems):
    copies = []
    for c in range(HALVES):
        copies.append([])
        for k, (ref, dst) in enumerate(zip(refs, dsts)):
            copy = pltpu.make_async_copy(
                ref.at[:, :, half(c)],
                dst.at[c, pl.ds(DEEP, NY), pl.ds(LEFT, NX), :],
                sems.at[c, k],
            )
            copy.start()
            copies[c].append(copy)
    return copies


def before_kernel(
    u_ref, f_ref, m_ref, e_lo, e_hi, n_lo, n_hi, c_lo, c_hi,
    u2_ref, cl_ref, cm_ref, cel, ceh, cnl, cnh, uel, ueh, unl, unh,
    us, fs, ms, ws, vs, pair, sems, out_sems,
):
    copies = fetch((u_ref, f_ref, m_ref), (us, fs, ms), sems)
    strips = (e_lo, e_hi, n_lo, n_hi, c_lo, c_hi)
    cells = corner_cells(INPUTS)
    outs = []
    for c in range(HALVES):
        h = half(c)
        u, f, m = us.at[c], fs.at[c], ms.at[c]
        for k, dst in enumerate((u, f, m)):
            place_halo(dst, h, FINE, *INPUTS[k], k, cells, *strips)
        for copy in copies[c]:
            copy.wait()
        two_sweeps(u, vs, f, m, ws)
        out = pltpu.make_async_copy(
            u.at[pl.ds(DEEP, NY), pl.ds(LEFT, NX), :], u2_ref.at[:, :, h], out_sems.at[c]
        )
        out.start()
        outs.append(out)

        def coarse_rows(i, carry):
            r = DEEP + 4 * i
            sums = {}
            for k, t, mid, s in stencil(u, r, LEFT, NX // 8, 4):
                at = pl.ds(LEFT + 8 * t, 8)
                mass = m[r + k, at, :]
                d = f[r + k, at, :] + s - (4.0 + mass) * mid
                if k % 2 == 0:
                    sums[t] = (d, mass)
                else:
                    pair[k // 2, 0, pl.ds(8 * t, 8), :] = sums[t][0] + d
                    pair[k // 2, 1, pl.ds(8 * t, 8), :] = sums[t][1] + mass
            for k in range(2):
                for which, ref in enumerate((cl_ref, cm_ref)):
                    ref[2 * i + k, :, h] = 0.5 * (
                        pair[k, which, pl.ds(0, CX, stride=2), :]
                        + pair[k, which, pl.ds(1, CX, stride=2), :]
                    )
            return carry

        lax.fori_loop(0, NY // 4, coarse_rows, 0)
        flat = u.reshape(FY * FX, LANES)
        for d in range(3):
            uel[d, :, h] = flat[pl.ds(DEEP * FX + LEFT + d, NY, stride=FX), :]
            ueh[d, :, h] = flat[pl.ds(DEEP * FX + LEFT + NX - 3 + d, NY, stride=FX), :]
            unl[d, :, h] = u[DEEP + d, pl.ds(LEFT, NX), :]
            unh[d, :, h] = u[NY + d, pl.ds(LEFT, NX), :]
    for d in range(WIDE):
        for k, ref in enumerate((cl_ref, cm_ref)):
            cel[k * WIDE + d] = ref[:, d, :]
            ceh[k * WIDE + d] = ref[:, CX - WIDE + d, :]
            cnl[k * WIDE + d] = ref[d]
            cnh[k * WIDE + d] = ref[CY - WIDE + d]
    for out in outs:
        out.wait()


def fine_scratch():
    both = VMEM((HALVES, FY, FX, LANES), F32)
    return [both] * 3 + [VMEM((FY, FX, LANES), F32)] * 2


def before(u, f, m, strips):
    return pl.pallas_call(
        before_kernel,
        out_shape=(shape(NY, NX, NC),)
        + (shape(CY, CX, NC),) * 2
        + (shape(2 * WIDE, CY, NC),) * 4
        + (shape(3, NY, NC),) * 4,
        in_specs=[IN_HBM] * 3 + [IN_VMEM] * 6,
        out_specs=(IN_HBM,) + (IN_VMEM,) * 10,
        scratch_shapes=fine_scratch()
        + [
            VMEM((2, 2, NX, LANES), F32),
            pltpu.SemaphoreType.DMA((HALVES, 3)),
            pltpu.SemaphoreType.DMA((HALVES,)),
        ],
        compiler_params=pltpu.CompilerParams(vmem_limit_bytes=40 * 2**20),
        name="before",
    )(u, f, m, *strips)


def coarse_kernel(
    cl_ref, cm_ref, e_lo, e_hi, n_lo, n_hi, c_lo, c_hi, uel, ueh, unl, unh,
    e_ref, ael, aeh, anl, anh,
    ls, ws, es, gs, tmp,
):
    cells = corner_cells(COARSE)
    rows, cols = pl.ds(TOP, CY), pl.ds(LEFT, CX)
    for c in range(HALVES):
        h = half(c)
        for k, (dst, ref) in enumerate(((ls, cl_ref), (ws, cm_ref))):
            dst[rows, cols, :] = ref[:, :, h]
            place_halo(
                dst, h, (TOP, CY, CX, GX), *COARSE[k], k, cells, e_lo, e_hi, n_lo, n_hi, c_lo, c_hi
            )
        wide = pl.ds(LEFT - 8, CX + 16)

        def first(i, carry):
            for k in range(BLOCK):
                r = TOP - WIDE + BLOCK * i + k
                w = 0.8 / (4.0 + ws[r, wide, :])
                ws[r, wide, :] = w
                es[r, wide, :] = w * ls[r, wide, :]
            return carry

        lax.fori_loop(0, (CY + 2 * WIDE) // BLOCK, first, 0)
        src, dst = es, gs
        for sweep in range(6):
            ring = 5 - sweep
            count = -(-(CY + 2 * ring) // BLOCK) * BLOCK
            sweep_rows(src, dst, ls, ws, TOP - ring, count, LEFT - 8, CX // 8 + 2)
            src, dst = dst, src
        e_ref[:, :, h] = src[rows, cols, :]
        flat = src.reshape(GY * GX, LANES)

        def spread(line):
            tmp[pl.ds(0, CX, stride=2), :] = line
            tmp[pl.ds(1, CX, stride=2), :] = line
            return tmp[...]

        for d in range(3):
            for out, old, x in ((ael, uel, d), (aeh, ueh, NX - 3 + d)):
                col = flat[pl.ds(TOP * GX + LEFT + x // 2, CY, stride=GX), :]
                out[d, :, h] = old[d, :, h] + spread(col)
            for out, old, y in ((anl, unl, d), (anh, unh, NY - 3 + d)):
                out[d, :, h] = old[d, :, h] + spread(src[TOP + y // 2, cols, :])


def coarse(load, mass, strips, u_strips):
    return pl.pallas_call(
        coarse_kernel,
        out_shape=(shape(CY, CX, NC),) + (shape(3, NY, NC),) * 4,
        in_specs=[IN_VMEM] * 12,
        out_specs=(IN_VMEM,) * 5,
        scratch_shapes=[VMEM((GY, GX, LANES), F32)] * 4 + [VMEM((NY, LANES), F32)],
        compiler_params=pltpu.CompilerParams(vmem_limit_bytes=24 * 2**20),
        name="coarse",
    )(load, mass, *strips, *u_strips)


def after_kernel(
    u_ref, f_ref, m_ref, e_ref, e_lo, e_hi, n_lo, n_hi, c_lo, c_hi,
    h_el, h_eh, h_nl, h_nh, h_cl, h_ch,
    out_ref, rest_ref,
    us, fs, ms, ws, vs, tmp, sems, out_sems,
):
    copies = fetch((u_ref, f_ref, m_ref), (us, fs, ms), sems)
    old = (h_el, h_eh, h_nl, h_nh, h_cl, h_ch)
    cells = corner_cells(INPUTS)
    outs = []
    for c in range(HALVES):
        h = half(c)
        u, f, m = us.at[c], fs.at[c], ms.at[c]
        mid = pl.ds(LEFT, NX)
        place_halo(
            u, h, FINE, *VALUES[0], 0, corner_cells(VALUES), e_lo, e_hi, n_lo, n_hi, c_lo, c_hi
        )
        for k, dst in ((1, f), (2, m)):
            place_halo(dst, h, FINE, *INPUTS[k], k, cells, *old)
        for copy in copies[c]:
            copy.wait()

        def add(i, carry):
            for k in range(4):
                line = e_ref[4 * i + k, :, h]
                tmp[k, pl.ds(0, CX, stride=2), :] = line
                tmp[k, pl.ds(1, CX, stride=2), :] = line
            for k in range(4):
                t = tmp[k]
                for j in range(2):
                    r = DEEP + 8 * i + 2 * k + j
                    u[r, mid, :] = u[r, mid, :] + t
            return carry

        lax.fori_loop(0, CY // 4, add, 0)
        two_sweeps(u, vs, f, m, ws)
        block = (pl.ds(DEEP, NY), mid)
        out = pltpu.make_async_copy(
            u.at[block[0], block[1], :], out_ref.at[:, :, h], out_sems.at[c, 0]
        )
        out.start()
        outs.append(out)

        def rest(i, carry):
            r = DEEP + BLOCK * i
            for k, t, value, s in stencil(u, r, LEFT, NX // 8, BLOCK):
                at = pl.ds(LEFT + 8 * t, 8)
                f[r + k, at, :] = f[r + k, at, :] + s - (4.0 + m[r + k, at, :]) * value
            return carry

        lax.fori_loop(0, NY // BLOCK, rest, 0)
        out = pltpu.make_async_copy(
            f.at[block[0], block[1], :], rest_ref.at[:, :, h], out_sems.at[c, 1]
        )
        out.start()
        outs.append(out)
    for out in outs:
        out.wait()


def after(u, f, m, e, strips, old):
    return pl.pallas_call(
        after_kernel,
        out_shape=(shape(NY, NX, NC),) * 2,
        in_specs=[IN_HBM] * 3 + [IN_VMEM] * 13,
        out_specs=(IN_HBM,) * 2,
        scratch_shapes=fine_scratch()
        + [
            VMEM((4, NX, LANES), F32),
            pltpu.SemaphoreType.DMA((HALVES, 3)),
            pltpu.SemaphoreType.DMA((HALVES, 2)),
        ],
        compiler_params=pltpu.CompilerParams(vmem_limit_bytes=40 * 2**20),
        name="after",
    )(u, f, m, e, *strips, *old)


def body(right_side, first_guess, mass_term):
    f, u, m = right_side, first_guess, mass_term
    old = halos(INPUTS, *edges(u, f, m))
    u2, load, mass, cel, ceh, cnl, cnh, *u_strips = before(u, f, m, old)
    wide = halos(COARSE, cel, ceh, cnl, cnh)
    e, *edge_values = coarse(load, mass, wide, u_strips)
    return after(u2, f, m, e, halos(VALUES, *edge_values), old)


def solution(mesh):
    spec = P("north", "east", None)
    return jax.shard_map(
        body, mesh=mesh, in_specs=(spec,) * 3, out_specs=(spec, spec), check_vma=False
    )
```

```python
import jax
import jax.numpy as jnp
from jax import lax
from jax.experimental import pallas as pl
from jax.experimental.pallas import tpu as pltpu
from jax.sharding import PartitionSpec as P

NY, NX, NC = 64, 64, 256
HALVES = 2
LANES = 128
DEEP = 3
LEFT = 16
FY, FX = NY + 2 * DEEP, NX + 2 * LEFT
CY, CX = NY // 2, NX // 2
WIDE = 6
TOP = 8
GY, GX = CY + 20, CX + 2 * LEFT
BLOCK = 4

VMEM = pltpu.VMEM
F32 = jnp.float32
IN_VMEM = pl.BlockSpec(memory_space=VMEM)
IN_HBM = pl.BlockSpec(memory_space=pltpu.HBM)

SLOT = 64
U1, U2, SWEPT, F1, M1 = range(5)
ENDS = 5 * SLOT
STRIP = ENDS + 8


FINE_CELLS = tuple(
    (side, slot * SLOT, n, k, dy)
    for k, slot, n, dy in ((0, U1, 2, 1), (0, U2, 1, 2), (1, F1, 1, 1), (2, M1, 1, 1))
    for side in range(2)
)
VALUE_CELLS = tuple(c for c in FINE_CELLS if c[3] == 0)
COARSE_CELLS = tuple(
    (side, (k * WIDE + (WIDE - dy if side == 0 else dy - 1)) * CX, WIDE - dy, k, dy)
    for k in range(2)
    for side in range(2)
    for dy in range(1, WIDE)
)


def half(c):
    return pl.ds(c * LANES, LANES)


def shape(*dims):
    return jax.ShapeDtypeStruct(dims, F32)


def exchange(low, high, axis):
    size = lax.axis_size(axis)
    up = [(i, (i + 1) % size) for i in range(size)]
    down = [(b, a) for a, b in up]
    return lax.ppermute(high, axis, up), lax.ppermute(low, axis, down)


def pack_kernel(cells, width, n_lo, n_hi, down, up):
    at = 0
    for side, row, n, _, _ in cells:
        src = (n_lo, n_hi)[side]
        down[pl.ds(at, n), :] = src[pl.ds(row, n), :]
        up[pl.ds(at, n), :] = src[pl.ds(row + width - n, n), :]
        at += n


def pack(cells, width, n_lo, n_hi):
    size = -(-sum(c[2] for c in cells) // 8) * 8
    return pl.pallas_call(
        lambda *refs: pack_kernel(cells, width, *refs),
        out_shape=(shape(size, NC),) * 2,
        in_specs=[IN_VMEM] * 2,
        out_specs=(IN_VMEM,) * 2,
        compiler_params=pltpu.CompilerParams(vmem_limit_bytes=7 * 2**20),
        name="pack",
    )(n_lo, n_hi)


def halos(cells, width, east_low, east_high, north_low, north_high):
    e_lo, e_hi = exchange(east_low, east_high, "east")
    n_lo, n_hi = exchange(north_low, north_high, "north")
    down, up = pack(cells, width, n_lo, n_hi)
    c_lo, c_hi = exchange(down, up, "east")
    return e_lo, e_hi, n_lo, n_hi, c_lo, c_hi


def weight_of(mass):
    return 0.8 / (4.0 + mass)


def swept_line(u1, u2, u3, f2, m2, line):
    line[pl.ds(8, SLOT), :] = u2
    s = (u1 + u3) + (line[pl.ds(7, SLOT), :] + line[pl.ds(9, SLOT), :]) + f2
    return 0.2 * u2 + weight_of(m2) * s


def clear_ends(line):
    line[pl.ds(0, 8), :] = jnp.zeros((8, LANES), F32)
    line[pl.ds(8 + SLOT, 8), :] = jnp.zeros((8, LANES), F32)


def write_strip(get, out, keep, line, h):
    u1, u2, u3, f2, m2 = get(0, 1), get(0, 2), get(0, 3), get(1, 2), get(2, 2)
    out[pl.ds(U1 * SLOT, SLOT), h] = u1
    out[pl.ds(U2 * SLOT, SLOT), h] = u2
    out[pl.ds(SWEPT * SLOT, SLOT), h] = swept_line(u1, u2, u3, f2, m2, line)
    out[pl.ds(F1 * SLOT, SLOT), h] = get(1, 1)
    out[pl.ds(M1 * SLOT, SLOT), h] = get(2, 1)
    keep[pl.ds(0, SLOT), h] = f2
    keep[pl.ds(SLOT, SLOT), h] = m2
    out[pl.ds(ENDS, 1), h] = keep[pl.ds(SLOT, 1), h]
    out[pl.ds(ENDS + 1, 1), h] = keep[pl.ds(2 * SLOT - 1, 1), h]
    out[pl.ds(ENDS + 2, 6), h] = jnp.zeros((6, LANES), F32)


def north_edges_kernel(u_ref, f_ref, m_ref, nl, nh, knl, knh, lines, line, sems):
    copies = []
    for side in range(2):
        for k, ref in enumerate((u_ref, f_ref, m_ref)):
            copy = pltpu.make_async_copy(
                ref.at[pl.ds(side * (NY - 3), 3)], lines.at[k, side], sems.at[k, side]
            )
            copy.start()
            copies.append(copy)
    clear_ends(line)
    for copy in copies:
        copy.wait()
    for side in range(2):
        for c in range(HALVES):
            h = half(c)
            write_strip(
                lambda k, d: lines[k, side, d - 1 if side == 0 else 3 - d, :, h],
                (nl, nh)[side], (knl, knh)[side], line, h,
            )


def east_edges_kernel(u_ref, f_ref, m_ref, el, eh, kel, keh, tiles, line, sems):
    copies = []
    for side in range(2):
        for c in range(HALVES):
            for k, ref in enumerate((u_ref, f_ref, m_ref)):
                copy = pltpu.make_async_copy(
                    ref.at[:, pl.ds(side * (NX - 8), 8), half(c)],
                    tiles.at[k, side, c],
                    sems.at[k, side, c],
                )
                copy.start()
                copies.append(copy)
    clear_ends(line)
    for copy in copies:
        copy.wait()
    for side in range(2):
        for c in range(HALVES):

            def get(k, d):
                flat = tiles.at[k, side, c].reshape(NY * 8, LANES)
                return flat[pl.ds(d - 1 if side == 0 else 8 - d, NY, stride=8), :]

            write_strip(get, (el, eh)[side], (kel, keh)[side], line, half(c))


def edges(kernel, buffer, sems, u, f, m):
    return pl.pallas_call(
        kernel,
        out_shape=(shape(STRIP, NC),) * 2 + (shape(2 * SLOT, NC),) * 2,
        in_specs=[IN_HBM] * 3,
        out_specs=(IN_VMEM,) * 4,
        scratch_shapes=[
            VMEM(buffer, F32),
            VMEM((SLOT + 16, LANES), F32),
            pltpu.SemaphoreType.DMA(sems),
        ],
        compiler_params=pltpu.CompilerParams(vmem_limit_bytes=58 * 2**20),
    )(u, f, m)


def mass_kernel(m_ref, low, high, tiles, pair, sems):
    copies = []
    for side in range(2):
        for c in range(HALVES):
            copy = pltpu.make_async_copy(
                m_ref.at[:, pl.ds(side * (NX - 16), 16), half(c)], tiles.at[side, c], sems.at[side, c]
            )
            copy.start()
            copies.append(copy)
    for side in range(2):
        for c in range(HALVES):
            copies[side * HALVES + c].wait()
            flat = tiles.at[side, c].reshape(NY * 16, LANES)
            for d in range(WIDE):
                x = 2 * d + (0 if side == 0 else 16 - 2 * WIDE)
                pair[...] = flat[pl.ds(x, NY, stride=16), :] + flat[pl.ds(x + 1, NY, stride=16), :]
                (low, high)[side][pl.ds(d * CY, CY), half(c)] = 0.5 * (
                    pair[pl.ds(0, CY, stride=2), :] + pair[pl.ds(1, CY, stride=2), :]
                )


def mass_columns(m):
    return pl.pallas_call(
        mass_kernel,
        out_shape=(shape(WIDE * CY, NC),) * 2,
        in_specs=[IN_HBM],
        out_specs=(IN_VMEM,) * 2,
        scratch_shapes=[
            VMEM((2, HALVES, NY, 16, LANES), F32),
            VMEM((NY, LANES), F32),
            pltpu.SemaphoreType.DMA((2, HALVES)),
        ],
        compiler_params=pltpu.CompilerParams(vmem_limit_bytes=16 * 2**20),
        name="mass_columns",
    )(m)


def place_corners(dst, h, sizes, array, cells, c_lo, c_hi, of=lambda x: x):
    top, ny, nx, _ = sizes
    where = 0
    for side, _, n, k, dy in cells:
        if k == array:
            row = top - dy if side == 0 else top + ny + dy - 1
            dst[row, pl.ds(LEFT - n, n), :] = of(c_lo[pl.ds(where, n), h])
            dst[row, pl.ds(LEFT + nx, n), :] = of(c_hi[pl.ds(where, n), h])
        where += n


def place_lines(dst, h, depth, slot, e_lo, e_hi, n_lo, n_hi, of=lambda x: x):
    flat = dst.reshape(FY * FX, LANES)
    at = pl.ds(slot * SLOT, SLOT)
    dst[DEEP - depth, pl.ds(LEFT, NX), :] = of(n_lo[at, h])
    dst[DEEP + NY + depth - 1, pl.ds(LEFT, NX), :] = of(n_hi[at, h])
    flat[pl.ds(DEEP * FX + LEFT - depth, NY, stride=FX), :] = of(e_lo[at, h])
    flat[pl.ds(DEEP * FX + LEFT + NX + depth - 1, NY, stride=FX), :] = of(e_hi[at, h])


FINE = (DEEP, NY, NX, FX)


def stencil(src, r, col, count, height):
    last = lax.broadcasted_iota(jnp.int32, (8, LANES), 0) == 7
    cache = {}

    def tile(k, t):
        if (k, t) not in cache:
            cache[k, t] = src[r + k, pl.ds(col + 8 * t, 8), :]
        return cache[k, t]

    turn = [pltpu.roll(tile(k, 0), 7, 0) for k in range(height)]
    for t in range(count):
        for k in range(height):
            following = pltpu.roll(tile(k, t + 1), 7, 0)
            right = jnp.where(last, following, turn[k])
            turn[k] = following
            left = src[r + k, pl.ds(col + 8 * t - 1, 8), :]
            yield k, t, tile(k, t), (tile(k - 1, t) + tile(k + 1, t)) + (left + right)


def sweep_rows(src, dst, load, weight, start, rows, col, count, mass=None):
    def block(i, carry):
        r = start + BLOCK * i
        for k, t, mid, s in stencil(src, r, col, count, BLOCK):
            at = pl.ds(col + 8 * t, 8)
            if mass is None:
                w = weight[r + k, at, :]
            else:
                w = 0.8 / (4.0 + mass[r + k, at, :])
                weight[r + k, at, :] = w
            dst[r + k, at, :] = 0.2 * mid + w * (s + load[r + k, at, :])
        return carry

    lax.fori_loop(0, rows // BLOCK, block, 0)


def two_sweeps(u, vs, f, ws, h, strips, ends, mass=None):
    args = (1, NY + 4, LEFT - 8, NX // 8 + 2)
    sweep_rows(u, vs, f, ws, *args, mass=mass)
    place_lines(vs, h, 2, SWEPT, *strips)
    low, high = DEEP, DEEP + NY - 1
    left, right = LEFT, LEFT + NX - 1
    e_lo, e_hi, n_lo, n_hi = ends

    def complete(row, col, from_row, from_col, mass):
        vs[row, pl.ds(col, 1), :] = (
            vs[row, pl.ds(col, 1), :] + weight_of(mass) * u[from_row, pl.ds(from_col, 1), :]
        )

    first, last = pl.ds(ENDS, 1), pl.ds(ENDS + 1, 1)
    for col, strip in ((left - 2, e_lo), (right + 2, e_hi)):
        complete(low, col, low - 1, col, strip[first, h])
        complete(high, col, high + 1, col, strip[last, h])
    for row, strip in ((low - 2, n_lo), (high + 2, n_hi)):
        complete(row, left, row, left - 1, strip[first, h])
        complete(row, right, row, right + 1, strip[last, h])
    sweep_rows(vs, u, f, ws, *args)


PADDED = (HALVES, FY, FX, LANES)


def load_kernel(u_ref, f_ref, m_ref, us, fs, ms, ws, sems):
    copies = {}
    for k, (ref, dst) in reversed(list(enumerate(((u_ref, us), (f_ref, fs), (m_ref, ms))))):
        for c in range(HALVES):
            copies[k, c] = pltpu.make_async_copy(
                ref.at[:, :, half(c)],
                dst.at[c, pl.ds(DEEP, NY), pl.ds(LEFT, NX), :],
                sems.at[k, c],
            )
            copies[k, c].start()
    for c in range(HALVES):
        copies[2, c].wait()

        def rows(i, carry):
            for k in range(BLOCK):
                at = (c, DEEP + BLOCK * i + k, pl.ds(LEFT, NX), slice(None))
                ws[at] = weight_of(ms[at])
            return carry

        lax.fori_loop(0, NY // BLOCK, rows, 0)
    for k in range(2):
        for c in range(HALVES):
            copies[k, c].wait()


def load(u, f, m):
    return pl.pallas_call(
        load_kernel,
        out_shape=(shape(*PADDED),) * 4,
        in_specs=[IN_HBM] * 3,
        out_specs=(IN_VMEM,) * 4,
        scratch_shapes=[pltpu.SemaphoreType.DMA((3, HALVES))],
        compiler_params=pltpu.CompilerParams(vmem_limit_bytes=7 * 2**20),
        cost_estimate=pl.CostEstimate(flops=2**26, bytes_accessed=12 * 2**20, transcendentals=0),
        name="load",
    )(u, f, m)


def before_kernel(
    _u, _f, _m, _w, e_lo, e_hi, n_lo, n_hi, c_lo, c_hi,
    us, fs, ms, ws, u2_ref, cl_ref, cm_ref, cel, ceh, cnl, cnh, uel, ueh, unl, unh,
    vs, pair,
):
    strips = (e_lo, e_hi, n_lo, n_hi)
    for c in range(HALVES):
        h = half(c)
        u, f, m, w = us.at[c], fs.at[c], ms.at[c], ws.at[c]
        for dst, depth, slot in ((u, 1, U1), (u, 2, U2), (f, 1, F1), (m, 1, M1)):
            place_lines(dst, h, depth, slot, *strips)
        place_lines(w, h, 1, M1, *strips, of=weight_of)
        for k, dst in enumerate((u, f, m)):
            place_corners(dst, h, FINE, k, FINE_CELLS, c_lo, c_hi)
        place_corners(w, h, FINE, 2, FINE_CELLS, c_lo, c_hi, of=weight_of)
        two_sweeps(u, vs, f, w, h, strips, strips)

        def coarse_rows(i, carry):
            r = DEEP + 4 * i
            sums = {}
            for k, t, mid, s in stencil(u, r, LEFT, NX // 8, 4):
                at = pl.ds(LEFT + 8 * t, 8)
                mass = m[r + k, at, :]
                u2_ref[4 * i + k, pl.ds(8 * t, 8), h] = mid
                d = f[r + k, at, :] + s - (4.0 + mass) * mid
                if k % 2 == 0:
                    sums[t] = (d, mass)
                else:
                    pair[k // 2, 0, pl.ds(8 * t, 8), :] = sums[t][0] + d
                    pair[k // 2, 1, pl.ds(8 * t, 8), :] = sums[t][1] + mass
            for k in range(2):
                for which, ref in enumerate((cl_ref, cm_ref)):
                    ref[2 * i + k, :, h] = 0.5 * (
                        pair[k, which, pl.ds(0, CX, stride=2), :]
                        + pair[k, which, pl.ds(1, CX, stride=2), :]
                    )
            return carry

        lax.fori_loop(0, NY // 4, coarse_rows, 0)
        flat = u.reshape(FY * FX, LANES)
        for d in range(3):
            at = pl.ds(d * SLOT, SLOT)
            uel[at, h] = flat[pl.ds(DEEP * FX + LEFT + d, NY, stride=FX), :]
            ueh[at, h] = flat[pl.ds(DEEP * FX + LEFT + NX - 1 - d, NY, stride=FX), :]
            unl[at, h] = u[DEEP + d, pl.ds(LEFT, NX), :]
            unh[at, h] = u[DEEP + NY - 1 - d, pl.ds(LEFT, NX), :]
    for d in range(WIDE):
        cel[pl.ds(d * CY, CY), :] = cl_ref[:, d, :]
        ceh[pl.ds(d * CY, CY), :] = cl_ref[:, CX - WIDE + d, :]
        for k, ref in enumerate((cl_ref, cm_ref)):
            at = pl.ds((k * WIDE + d) * CX, CX)
            cnl[at, :] = ref[d]
            cnh[at, :] = ref[CY - WIDE + d]


def before(padded, strips):
    return pl.pallas_call(
        before_kernel,
        out_shape=(shape(*PADDED),) * 4
        + (shape(NY, NX, NC),)
        + (shape(CY, CX, NC),) * 2
        + (shape(WIDE * CY, NC),) * 2
        + (shape(2 * WIDE * CX, NC),) * 2
        + (shape(3 * SLOT, NC),) * 4,
        in_specs=[IN_VMEM] * 10,
        out_specs=(IN_VMEM,) * 15,
        input_output_aliases={k: k for k in range(4)},
        scratch_shapes=[VMEM((FY, FX, LANES), F32), VMEM((2, 2, NX, LANES), F32)],
        compiler_params=pltpu.CompilerParams(vmem_limit_bytes=7 * 2**20),
        name="before",
    )(*padded, *strips)


def coarse_kernel(
    cl_ref, cm_ref, me_lo, me_hi, e_lo, e_hi, n_lo, n_hi, c_lo, c_hi,
    uel, ueh, unl, unh, kel, keh, knl, knh,
    e_ref, ael, aeh, anl, anh,
    ls, ws, es, gs, tmp, line,
):
    rows, cols = pl.ds(TOP, CY), pl.ds(LEFT, CX)
    clear_ends(line)
    for c in range(HALVES):
        h = half(c)
        for k, (dst, ref, lo, hi) in enumerate(
            ((ls, cl_ref, e_lo, e_hi), (ws, cm_ref, me_lo, me_hi))
        ):
            dst[rows, cols, :] = ref[:, :, h]
            flat = dst.reshape(GY * GX, LANES)
            for d in range(WIDE):
                at = pl.ds((k * WIDE + d) * CX, CX)
                dst[TOP - WIDE + d, cols, :] = n_lo[at, h]
                dst[TOP + CY + d, cols, :] = n_hi[at, h]
                at = pl.ds(d * CY, CY)
                flat[pl.ds(TOP * GX + LEFT - WIDE + d, CY, stride=GX), :] = lo[at, h]
                flat[pl.ds(TOP * GX + LEFT + CX + d, CY, stride=GX), :] = hi[at, h]
            place_corners(dst, h, (TOP, CY, CX, GX), k, COARSE_CELLS, c_lo, c_hi)
        wide = pl.ds(LEFT - 8, CX + 16)

        def first(i, carry):
            for k in range(BLOCK):
                r = TOP - WIDE + BLOCK * i + k
                w = 0.8 / (4.0 + ws[r, wide, :])
                ws[r, wide, :] = w
                es[r, wide, :] = w * ls[r, wide, :]
            return carry

        lax.fori_loop(0, (CY + 2 * WIDE) // BLOCK, first, 0)
        src, dst = es, gs
        for sweep in range(6):
            ring = 5 - sweep
            count = -(-(CY + 2 * ring) // BLOCK) * BLOCK
            sweep_rows(src, dst, ls, ws, TOP - ring, count, LEFT - 8, CX // 8 + 2)
            src, dst = dst, src
        e_ref[:, :, h] = src[rows, cols, :]
        flat = src.reshape(GY * GX, LANES)

        def spread(line):
            tmp[pl.ds(0, CX, stride=2), :] = line
            tmp[pl.ds(1, CX, stride=2), :] = line
            return tmp[...]

        for out, old, keep, where, high in (
            (ael, uel, kel, "x", False), (aeh, ueh, keh, "x", True),
            (anl, unl, knl, "y", False), (anh, unh, knh, "y", True),
        ):
            values = []
            for d in range(3):
                at = (CX - 1 - d // 2) if high else d // 2
                if where == "x":
                    coarse_line = flat[pl.ds(TOP * GX + LEFT + at, CY, stride=GX), :]
                else:
                    coarse_line = src[TOP + at, cols, :]
                values.append(old[pl.ds(d * SLOT, SLOT), h] + spread(coarse_line))
            f2, m2 = keep[pl.ds(0, SLOT), h], keep[pl.ds(SLOT, SLOT), h]
            out[pl.ds(U1 * SLOT, SLOT), h] = values[0]
            out[pl.ds(U2 * SLOT, SLOT), h] = values[1]
            out[pl.ds(SWEPT * SLOT, SLOT), h] = swept_line(*values, f2, m2, line)


def coarse(right, mass, mass_strips, strips, u_strips, kept):
    return pl.pallas_call(
        coarse_kernel,
        out_shape=(shape(CY, CX, NC),) + (shape(3 * SLOT, NC),) * 4,
        in_specs=[IN_VMEM] * 18,
        out_specs=(IN_VMEM,) * 5,
        scratch_shapes=[VMEM((GY, GX, LANES), F32)] * 4
        + [VMEM((NY, LANES), F32), VMEM((SLOT + 16, LANES), F32)],
        compiler_params=pltpu.CompilerParams(vmem_limit_bytes=7 * 2**20),
        name="coarse",
    )(right, mass, *mass_strips, *strips, *u_strips, *kept)


def fetch(refs, dsts, sems):
    copies = []
    for c in range(HALVES):
        copies.append([])
        for k, (ref, dst) in enumerate(zip(refs, dsts)):
            copy = pltpu.make_async_copy(
                ref.at[:, :, half(c)],
                dst.at[c, pl.ds(DEEP, NY), pl.ds(LEFT, NX), :],
                sems.at[c, k],
            )
            copy.start()
            copies[c].append(copy)
    return copies


def fine_scratch():
    both = VMEM((HALVES, FY, FX, LANES), F32)
    return [both] * 3 + [VMEM((FY, FX, LANES), F32)] * 2


def after_kernel(
    u_ref, f_ref, m_ref, e_ref, e_lo, e_hi, n_lo, n_hi, c_lo, c_hi,
    h_el, h_eh, h_nl, h_nh, h_cl, h_ch,
    out_ref, rest_ref,
    us, fs, ms, ws, vs, tmp, sems, out_sems,
):
    copies = fetch((u_ref, f_ref, m_ref), (us, fs, ms), sems)
    strips, old = (e_lo, e_hi, n_lo, n_hi), (h_el, h_eh, h_nl, h_nh)
    outs = []
    for c in range(HALVES):
        h = half(c)
        u, f, m = us.at[c], fs.at[c], ms.at[c]
        mid = pl.ds(LEFT, NX)
        place_lines(u, h, 1, U1, *strips)
        place_lines(u, h, 2, U2, *strips)
        place_corners(u, h, FINE, 0, VALUE_CELLS, c_lo, c_hi)
        for k, dst, slot in ((1, f, F1), (2, m, M1)):
            place_lines(dst, h, 1, slot, *old)
            place_corners(dst, h, FINE, k, FINE_CELLS, h_cl, h_ch)
        for copy in copies[c]:
            copy.wait()

        def add(i, carry):
            for k in range(4):
                line = e_ref[4 * i + k, :, h]
                tmp[k, pl.ds(0, CX, stride=2), :] = line
                tmp[k, pl.ds(1, CX, stride=2), :] = line
            for k in range(4):
                t = tmp[k]
                for j in range(2):
                    r = DEEP + 8 * i + 2 * k + j
                    u[r, mid, :] = u[r, mid, :] + t
            return carry

        lax.fori_loop(0, CY // 4, add, 0)
        two_sweeps(u, vs, f, ws, h, strips, old, mass=m)
        block = (pl.ds(DEEP, NY), mid)
        out = pltpu.make_async_copy(
            u.at[block[0], block[1], :], out_ref.at[:, :, h], out_sems.at[c, 0]
        )
        out.start()
        outs.append(out)

        def rest(i, carry):
            r = DEEP + BLOCK * i
            for k, t, value, s in stencil(u, r, LEFT, NX // 8, BLOCK):
                at = pl.ds(LEFT + 8 * t, 8)
                f[r + k, at, :] = f[r + k, at, :] + s - (4.0 + m[r + k, at, :]) * value
            return carry

        lax.fori_loop(0, NY // BLOCK, rest, 0)
        out = pltpu.make_async_copy(
            f.at[block[0], block[1], :], rest_ref.at[:, :, h], out_sems.at[c, 1]
        )
        out.start()
        outs.append(out)
    for out in outs:
        out.wait()


def after(u, f, m, e, strips, old):
    return pl.pallas_call(
        after_kernel,
        out_shape=(shape(NY, NX, NC),) * 2,
        in_specs=[IN_HBM] * 3 + [IN_VMEM] * 13,
        out_specs=(IN_HBM,) * 2,
        scratch_shapes=fine_scratch()
        + [
            VMEM((4, NX, LANES), F32),
            pltpu.SemaphoreType.DMA((HALVES, 3)),
            pltpu.SemaphoreType.DMA((HALVES, 2)),
        ],
        compiler_params=pltpu.CompilerParams(vmem_limit_bytes=40 * 2**20),
        name="after",
    )(u, f, m, e, *strips, *old)


def body(right_side, first_guess, mass_term):
    f, u, m = right_side, first_guess, mass_term
    nl, nh, *north_kept = edges(north_edges_kernel, (3, 2, 3, NX, NC), (3, 2), u, f, m)
    el, eh, *kept = edges(east_edges_kernel, (3, 2, HALVES, NY, 8, LANES), (3, 2, HALVES), u, f, m)
    kept += north_kept
    old = halos(FINE_CELLS, NX, el, eh, nl, nh)
    columns = mass_columns(m)
    padded = load(u, f, m)
    mass_strips = exchange(*columns, "east")
    _, _, _, _, u2, right, mass, cel, ceh, cnl, cnh, *u_strips = before(padded, old)
    wide = halos(COARSE_CELLS, CX, cel, ceh, cnl, cnh)
    e, *edge_values = coarse(right, mass, mass_strips, wide, u_strips, kept)
    strips = halos(VALUE_CELLS, NX, *edge_values)
    return after(u2, f, m, e, strips, old)


def solution(mesh):
    spec = P("north", "east", None)
    return jax.shard_map(
        body, mesh=mesh, in_specs=(spec,) * 3, out_specs=(spec, spec), check_vma=False
    )
```

```python
import jax
import jax.numpy as jnp
from jax import lax
from jax.experimental import pallas as pl
from jax.experimental.pallas import tpu as pltpu
from jax.sharding import PartitionSpec as P

NY, NX, NC = 64, 64, 256
HALVES = 2
LANES = 128
DEEP = 3
LEFT = 16
FY, FX = NY + 2 * DEEP, NX + 2 * LEFT
CY, CX = NY // 2, NX // 2
WIDE = 6
TOP = 8
GY, GX = CY + 20, CX + 2 * LEFT
BLOCK = 4

VMEM = pltpu.VMEM
F32 = jnp.float32
IN_VMEM = pl.BlockSpec(memory_space=VMEM)
IN_HBM = pl.BlockSpec(memory_space=pltpu.HBM)

SLOT = 64
U1, U2, SWEPT, F1, M1 = range(5)
ENDS = 5 * SLOT
STRIP = ENDS + 8


FINE_CELLS = tuple(
    (side, slot * SLOT, n, k, dy)
    for k, slot, n, dy in ((0, U1, 2, 1), (0, U2, 1, 2), (1, F1, 1, 1), (2, M1, 1, 1))
    for side in range(2)
)
VALUE_CELLS = tuple(c for c in FINE_CELLS if c[3] == 0)
COARSE_CELLS = tuple(
    (side, (k * WIDE + (WIDE - dy if side == 0 else dy - 1)) * CX, WIDE - dy, k, dy)
    for k in range(2)
    for side in range(2)
    for dy in range(1, WIDE)
)


def half(c):
    return pl.ds(c * LANES, LANES)


def shape(*dims):
    return jax.ShapeDtypeStruct(dims, F32)


def exchange(low, high, axis):
    size = lax.axis_size(axis)
    up = [(i, (i + 1) % size) for i in range(size)]
    down = [(b, a) for a, b in up]
    return lax.ppermute(high, axis, up), lax.ppermute(low, axis, down)


def pack_kernel(cells, width, n_lo, n_hi, down, up):
    at = 0
    for side, row, n, _, _ in cells:
        src = (n_lo, n_hi)[side]
        down[pl.ds(at, n), :] = src[pl.ds(row, n), :]
        up[pl.ds(at, n), :] = src[pl.ds(row + width - n, n), :]
        at += n


def pack(cells, width, n_lo, n_hi):
    size = -(-sum(c[2] for c in cells) // 8) * 8
    return pl.pallas_call(
        lambda *refs: pack_kernel(cells, width, *refs),
        out_shape=(shape(size, NC),) * 2,
        in_specs=[IN_VMEM] * 2,
        out_specs=(IN_VMEM,) * 2,
        compiler_params=pltpu.CompilerParams(vmem_limit_bytes=7 * 2**20),
        name="pack",
    )(n_lo, n_hi)


def halos(cells, width, east_low, east_high, north_low, north_high):
    e_lo, e_hi = exchange(east_low, east_high, "east")
    n_lo, n_hi = exchange(north_low, north_high, "north")
    down, up = pack(cells, width, n_lo, n_hi)
    c_lo, c_hi = exchange(down, up, "east")
    return e_lo, e_hi, n_lo, n_hi, c_lo, c_hi


def weight_of(mass):
    return 0.8 / (4.0 + mass)


def swept_line(u1, u2, u3, f2, m2, line):
    line[pl.ds(8, SLOT), :] = u2
    s = (u1 + u3) + (line[pl.ds(7, SLOT), :] + line[pl.ds(9, SLOT), :]) + f2
    return 0.2 * u2 + weight_of(m2) * s


def clear_ends(line):
    line[pl.ds(0, 8), :] = jnp.zeros((8, LANES), F32)
    line[pl.ds(8 + SLOT, 8), :] = jnp.zeros((8, LANES), F32)


def write_strip(get, out, keep, line, h):
    u1, u2, u3, f2, m2 = get(0, 1), get(0, 2), get(0, 3), get(1, 2), get(2, 2)
    out[pl.ds(U1 * SLOT, SLOT), h] = u1
    out[pl.ds(U2 * SLOT, SLOT), h] = u2
    out[pl.ds(SWEPT * SLOT, SLOT), h] = swept_line(u1, u2, u3, f2, m2, line)
    out[pl.ds(F1 * SLOT, SLOT), h] = get(1, 1)
    out[pl.ds(M1 * SLOT, SLOT), h] = get(2, 1)
    keep[pl.ds(0, SLOT), h] = f2
    keep[pl.ds(SLOT, SLOT), h] = m2
    out[pl.ds(ENDS, 1), h] = keep[pl.ds(SLOT, 1), h]
    out[pl.ds(ENDS + 1, 1), h] = keep[pl.ds(2 * SLOT - 1, 1), h]
    out[pl.ds(ENDS + 2, 6), h] = jnp.zeros((6, LANES), F32)


def north_edges_kernel(
    u_ref, f_ref, m_ref, nl, nh, knl, knh, tiles, lines, line, sems, tile_sems
):
    copies, tile_copies = [], []
    for side in range(2):
        for k, ref in enumerate((u_ref, f_ref, m_ref)):
            copy = pltpu.make_async_copy(
                ref.at[pl.ds(side * (NY - 3), 3)], lines.at[k, side], sems.at[k, side]
            )
            copy.start()
            copies.append(copy)
    for side in range(2):
        for c in range(HALVES):
            for k, ref in enumerate((u_ref, f_ref, m_ref)):
                copy = pltpu.make_async_copy(
                    ref.at[:, pl.ds(side * (NX - 8), 8), half(c)],
                    tiles.at[k, side, c],
                    tile_sems.at[k, side, c],
                )
                copy.start()
                tile_copies.append(copy)
    clear_ends(line)
    for copy in copies:
        copy.wait()
    for side in range(2):
        for c in range(HALVES):
            h = half(c)
            write_strip(
                lambda k, d: lines[k, side, d - 1 if side == 0 else 3 - d, :, h],
                (nl, nh)[side], (knl, knh)[side], line, h,
            )
    for copy in tile_copies:
        copy.wait()


def east_edges_kernel(tiles, el, eh, kel, keh, line):
    clear_ends(line)
    for side in range(2):
        for c in range(HALVES):

            def get(k, d):
                flat = tiles.at[k, side, c].reshape(NY * 8, LANES)
                return flat[pl.ds(d - 1 if side == 0 else 8 - d, NY, stride=8), :]

            write_strip(get, (el, eh)[side], (kel, keh)[side], line, half(c))


STRIPS = (shape(STRIP, NC),) * 2 + (shape(2 * SLOT, NC),) * 2
TILES = (3, 2, HALVES, NY, 8, LANES)


def north_edges(u, f, m):
    return pl.pallas_call(
        north_edges_kernel,
        out_shape=STRIPS + (shape(*TILES),),
        in_specs=[IN_HBM] * 3,
        out_specs=(IN_VMEM,) * 5,
        scratch_shapes=[
            VMEM((3, 2, 3, NX, NC), F32),
            VMEM((SLOT + 16, LANES), F32),
            pltpu.SemaphoreType.DMA((3, 2)),
            pltpu.SemaphoreType.DMA((3, 2, HALVES)),
        ],
        compiler_params=pltpu.CompilerParams(vmem_limit_bytes=48 * 2**20),
        name="north_edges",
    )(u, f, m)


def east_edges(tiles):
    return pl.pallas_call(
        east_edges_kernel,
        out_shape=STRIPS,
        in_specs=[IN_VMEM],
        out_specs=(IN_VMEM,) * 4,
        scratch_shapes=[VMEM((SLOT + 16, LANES), F32)],
        compiler_params=pltpu.CompilerParams(vmem_limit_bytes=8 * 2**20),
        name="east_edges",
    )(tiles)


def mass_kernel(m_ref, low, high, tiles, pair, sems):
    copies = []
    for side in range(2):
        for c in range(HALVES):
            copy = pltpu.make_async_copy(
                m_ref.at[:, pl.ds(side * (NX - 16), 16), half(c)], tiles.at[side, c], sems.at[side, c]
            )
            copy.start()
            copies.append(copy)
    for side in range(2):
        for c in range(HALVES):
            copies[side * HALVES + c].wait()
            flat = tiles.at[side, c].reshape(NY * 16, LANES)
            for d in range(WIDE):
                x = 2 * d + (0 if side == 0 else 16 - 2 * WIDE)
                pair[...] = flat[pl.ds(x, NY, stride=16), :] + flat[pl.ds(x + 1, NY, stride=16), :]
                (low, high)[side][pl.ds(d * CY, CY), half(c)] = 0.5 * (
                    pair[pl.ds(0, CY, stride=2), :] + pair[pl.ds(1, CY, stride=2), :]
                )


def mass_columns(m):
    return pl.pallas_call(
        mass_kernel,
        out_shape=(shape(WIDE * CY, NC),) * 2,
        in_specs=[IN_HBM],
        out_specs=(IN_VMEM,) * 2,
        scratch_shapes=[
            VMEM((2, HALVES, NY, 16, LANES), F32),
            VMEM((NY, LANES), F32),
            pltpu.SemaphoreType.DMA((2, HALVES)),
        ],
        compiler_params=pltpu.CompilerParams(vmem_limit_bytes=16 * 2**20),
        name="mass_columns",
    )(m)


def place_corners(dst, h, sizes, array, cells, c_lo, c_hi, of=lambda x: x):
    top, ny, nx, _ = sizes
    where = 0
    for side, _, n, k, dy in cells:
        if k == array:
            row = top - dy if side == 0 else top + ny + dy - 1
            dst[row, pl.ds(LEFT - n, n), :] = of(c_lo[pl.ds(where, n), h])
            dst[row, pl.ds(LEFT + nx, n), :] = of(c_hi[pl.ds(where, n), h])
        where += n


def place_lines(dst, h, depth, slot, e_lo, e_hi, n_lo, n_hi, of=lambda x: x):
    flat = dst.reshape(FY * FX, LANES)
    at = pl.ds(slot * SLOT, SLOT)
    dst[DEEP - depth, pl.ds(LEFT, NX), :] = of(n_lo[at, h])
    dst[DEEP + NY + depth - 1, pl.ds(LEFT, NX), :] = of(n_hi[at, h])
    flat[pl.ds(DEEP * FX + LEFT - depth, NY, stride=FX), :] = of(e_lo[at, h])
    flat[pl.ds(DEEP * FX + LEFT + NX + depth - 1, NY, stride=FX), :] = of(e_hi[at, h])


FINE = (DEEP, NY, NX, FX)


def stencil(src, r, col, count, height):
    last = lax.broadcasted_iota(jnp.int32, (8, LANES), 0) == 7
    cache = {}

    def tile(k, t):
        if (k, t) not in cache:
            cache[k, t] = src[r + k, pl.ds(col + 8 * t, 8), :]
        return cache[k, t]

    turn = [pltpu.roll(tile(k, 0), 7, 0) for k in range(height)]
    for t in range(count):
        for k in range(height):
            following = pltpu.roll(tile(k, t + 1), 7, 0)
            right = jnp.where(last, following, turn[k])
            turn[k] = following
            left = src[r + k, pl.ds(col + 8 * t - 1, 8), :]
            yield k, t, tile(k, t), (tile(k - 1, t) + tile(k + 1, t)) + (left + right)


def sweep_rows(src, dst, load, weight, start, rows, col, count, mass=None):
    def block(i, carry):
        r = start + BLOCK * i
        for k, t, mid, s in stencil(src, r, col, count, BLOCK):
            at = pl.ds(col + 8 * t, 8)
            if mass is None:
                w = weight[r + k, at, :]
            else:
                w = 0.8 / (4.0 + mass[r + k, at, :])
                weight[r + k, at, :] = w
            dst[r + k, at, :] = 0.2 * mid + w * (s + load[r + k, at, :])
        return carry

    lax.fori_loop(0, rows // BLOCK, block, 0)


def two_sweeps(u, vs, f, ws, h, strips, ends, mass=None):
    args = (1, NY + 4, LEFT - 8, NX // 8 + 2)
    sweep_rows(u, vs, f, ws, *args, mass=mass)
    place_lines(vs, h, 2, SWEPT, *strips)
    low, high = DEEP, DEEP + NY - 1
    left, right = LEFT, LEFT + NX - 1
    e_lo, e_hi, n_lo, n_hi = ends

    def complete(row, col, from_row, from_col, mass):
        vs[row, pl.ds(col, 1), :] = (
            vs[row, pl.ds(col, 1), :] + weight_of(mass) * u[from_row, pl.ds(from_col, 1), :]
        )

    first, last = pl.ds(ENDS, 1), pl.ds(ENDS + 1, 1)
    for col, strip in ((left - 2, e_lo), (right + 2, e_hi)):
        complete(low, col, low - 1, col, strip[first, h])
        complete(high, col, high + 1, col, strip[last, h])
    for row, strip in ((low - 2, n_lo), (high + 2, n_hi)):
        complete(row, left, row, left - 1, strip[first, h])
        complete(row, right, row, right + 1, strip[last, h])
    sweep_rows(vs, u, f, ws, *args)


PADDED = (HALVES, FY, FX, LANES)


def load_kernel(u_ref, f_ref, m_ref, us, fs, ms, ws, sems):
    copies = {}
    for k, (ref, dst) in reversed(list(enumerate(((u_ref, us), (f_ref, fs), (m_ref, ms))))):
        for c in range(HALVES):
            copies[k, c] = pltpu.make_async_copy(
                ref.at[:, :, half(c)],
                dst.at[c, pl.ds(DEEP, NY), pl.ds(LEFT, NX), :],
                sems.at[k, c],
            )
            copies[k, c].start()
    for c in range(HALVES):
        copies[2, c].wait()

        def rows(i, carry):
            for k in range(BLOCK):
                at = (c, DEEP + BLOCK * i + k, pl.ds(LEFT, NX), slice(None))
                ws[at] = weight_of(ms[at])
            return carry

        lax.fori_loop(0, NY // BLOCK, rows, 0)
    for k in range(2):
        for c in range(HALVES):
            copies[k, c].wait()


def load(u, f, m):
    return pl.pallas_call(
        load_kernel,
        out_shape=(shape(*PADDED),) * 4,
        in_specs=[IN_HBM] * 3,
        out_specs=(IN_VMEM,) * 4,
        scratch_shapes=[pltpu.SemaphoreType.DMA((3, HALVES))],
        compiler_params=pltpu.CompilerParams(vmem_limit_bytes=7 * 2**20),
        cost_estimate=pl.CostEstimate(flops=2**26, bytes_accessed=12 * 2**20, transcendentals=0),
        name="load",
    )(u, f, m)


def before_kernel(
    _u, _f, _m, _w, e_lo, e_hi, n_lo, n_hi, c_lo, c_hi,
    us, fs, ms, ws, u2_ref, cl_ref, cm_ref, cel, ceh, cnl, cnh, uel, ueh, unl, unh,
    vs, pair,
):
    strips = (e_lo, e_hi, n_lo, n_hi)
    for c in range(HALVES):
        h = half(c)
        u, f, m, w = us.at[c], fs.at[c], ms.at[c], ws.at[c]
        for dst, depth, slot in ((u, 1, U1), (u, 2, U2), (f, 1, F1), (m, 1, M1)):
            place_lines(dst, h, depth, slot, *strips)
        place_lines(w, h, 1, M1, *strips, of=weight_of)
        for k, dst in enumerate((u, f, m)):
            place_corners(dst, h, FINE, k, FINE_CELLS, c_lo, c_hi)
        place_corners(w, h, FINE, 2, FINE_CELLS, c_lo, c_hi, of=weight_of)
        two_sweeps(u, vs, f, w, h, strips, strips)

        def coarse_rows(i, carry):
            r = DEEP + 4 * i
            sums = {}
            for k, t, mid, s in stencil(u, r, LEFT, NX // 8, 4):
                at = pl.ds(LEFT + 8 * t, 8)
                mass = m[r + k, at, :]
                u2_ref[4 * i + k, pl.ds(8 * t, 8), h] = mid
                d = f[r + k, at, :] + s - (4.0 + mass) * mid
                if k % 2 == 0:
                    sums[t] = (d, mass)
                else:
                    pair[k // 2, 0, pl.ds(8 * t, 8), :] = sums[t][0] + d
                    pair[k // 2, 1, pl.ds(8 * t, 8), :] = sums[t][1] + mass
            for k in range(2):
                for which, ref in enumerate((cl_ref, cm_ref)):
                    ref[2 * i + k, :, h] = 0.5 * (
                        pair[k, which, pl.ds(0, CX, stride=2), :]
                        + pair[k, which, pl.ds(1, CX, stride=2), :]
                    )
            return carry

        lax.fori_loop(0, NY // 4, coarse_rows, 0)
        flat = u.reshape(FY * FX, LANES)
        for d in range(3):
            at = pl.ds(d * SLOT, SLOT)
            uel[at, h] = flat[pl.ds(DEEP * FX + LEFT + d, NY, stride=FX), :]
            ueh[at, h] = flat[pl.ds(DEEP * FX + LEFT + NX - 1 - d, NY, stride=FX), :]
            unl[at, h] = u[DEEP + d, pl.ds(LEFT, NX), :]
            unh[at, h] = u[DEEP + NY - 1 - d, pl.ds(LEFT, NX), :]
    for d in range(WIDE):
        cel[pl.ds(d * CY, CY), :] = cl_ref[:, d, :]
        ceh[pl.ds(d * CY, CY), :] = cl_ref[:, CX - WIDE + d, :]
        for k, ref in enumerate((cl_ref, cm_ref)):
            at = pl.ds((k * WIDE + d) * CX, CX)
            cnl[at, :] = ref[d]
            cnh[at, :] = ref[CY - WIDE + d]


def before(padded, strips):
    return pl.pallas_call(
        before_kernel,
        out_shape=(shape(*PADDED),) * 4
        + (shape(NY, NX, NC),)
        + (shape(CY, CX, NC),) * 2
        + (shape(WIDE * CY, NC),) * 2
        + (shape(2 * WIDE * CX, NC),) * 2
        + (shape(3 * SLOT, NC),) * 4,
        in_specs=[IN_VMEM] * 10,
        out_specs=(IN_VMEM,) * 15,
        input_output_aliases={k: k for k in range(4)},
        scratch_shapes=[VMEM((FY, FX, LANES), F32), VMEM((2, 2, NX, LANES), F32)],
        compiler_params=pltpu.CompilerParams(vmem_limit_bytes=9 * 2**20),
        name="before",
    )(*padded, *strips)


def coarse_kernel(
    cl_ref, cm_ref, me_lo, me_hi, e_lo, e_hi, n_lo, n_hi, c_lo, c_hi,
    uel, ueh, unl, unh, kel, keh, knl, knh,
    e_ref, ael, aeh, anl, anh,
    ls, ws, es, gs, tmp, line,
):
    rows, cols = pl.ds(TOP, CY), pl.ds(LEFT, CX)
    clear_ends(line)
    for c in range(HALVES):
        h = half(c)
        for k, (dst, ref, lo, hi) in enumerate(
            ((ls, cl_ref, e_lo, e_hi), (ws, cm_ref, me_lo, me_hi))
        ):
            dst[rows, cols, :] = ref[:, :, h]
            flat = dst.reshape(GY * GX, LANES)
            for d in range(WIDE):
                at = pl.ds((k * WIDE + d) * CX, CX)
                dst[TOP - WIDE + d, cols, :] = n_lo[at, h]
                dst[TOP + CY + d, cols, :] = n_hi[at, h]
                at = pl.ds(d * CY, CY)
                flat[pl.ds(TOP * GX + LEFT - WIDE + d, CY, stride=GX), :] = lo[at, h]
                flat[pl.ds(TOP * GX + LEFT + CX + d, CY, stride=GX), :] = hi[at, h]
            place_corners(dst, h, (TOP, CY, CX, GX), k, COARSE_CELLS, c_lo, c_hi)
        wide = pl.ds(LEFT - 8, CX + 16)

        def first(i, carry):
            for k in range(BLOCK):
                r = TOP - WIDE + BLOCK * i + k
                w = 0.8 / (4.0 + ws[r, wide, :])
                ws[r, wide, :] = w
                es[r, wide, :] = w * ls[r, wide, :]
            return carry

        lax.fori_loop(0, (CY + 2 * WIDE) // BLOCK, first, 0)
        src, dst = es, gs
        for sweep in range(6):
            ring = 5 - sweep
            count = -(-(CY + 2 * ring) // BLOCK) * BLOCK
            sweep_rows(src, dst, ls, ws, TOP - ring, count, LEFT - 8, CX // 8 + 2)
            src, dst = dst, src
        e_ref[:, :, h] = src[rows, cols, :]
        flat = src.reshape(GY * GX, LANES)

        def spread(line):
            tmp[pl.ds(0, CX, stride=2), :] = line
            tmp[pl.ds(1, CX, stride=2), :] = line
            return tmp[...]

        for out, old, keep, where, high in (
            (ael, uel, kel, "x", False), (aeh, ueh, keh, "x", True),
            (anl, unl, knl, "y", False), (anh, unh, knh, "y", True),
        ):
            values = []
            for d in range(3):
                at = (CX - 1 - d // 2) if high else d // 2
                if where == "x":
                    coarse_line = flat[pl.ds(TOP * GX + LEFT + at, CY, stride=GX), :]
                else:
                    coarse_line = src[TOP + at, cols, :]
                values.append(old[pl.ds(d * SLOT, SLOT), h] + spread(coarse_line))
            f2, m2 = keep[pl.ds(0, SLOT), h], keep[pl.ds(SLOT, SLOT), h]
            out[pl.ds(U1 * SLOT, SLOT), h] = values[0]
            out[pl.ds(U2 * SLOT, SLOT), h] = values[1]
            out[pl.ds(SWEPT * SLOT, SLOT), h] = swept_line(*values, f2, m2, line)


def coarse(right, mass, mass_strips, strips, u_strips, kept):
    return pl.pallas_call(
        coarse_kernel,
        out_shape=(shape(CY, CX, NC),) + (shape(3 * SLOT, NC),) * 4,
        in_specs=[IN_VMEM] * 18,
        out_specs=(IN_VMEM,) * 5,
        scratch_shapes=[VMEM((GY, GX, LANES), F32)] * 4
        + [VMEM((NY, LANES), F32), VMEM((SLOT + 16, LANES), F32)],
        compiler_params=pltpu.CompilerParams(vmem_limit_bytes=9 * 2**20),
        name="coarse",
    )(right, mass, *mass_strips, *strips, *u_strips, *kept)


def fetch(refs, dsts, sems):
    copies = []
    for c in range(HALVES):
        copies.append([])
        for k, (ref, dst) in enumerate(zip(refs, dsts)):
            copy = pltpu.make_async_copy(
                ref.at[:, :, half(c)],
                dst.at[c, pl.ds(DEEP, NY), pl.ds(LEFT, NX), :],
                sems.at[c, k],
            )
            copy.start()
            copies[c].append(copy)
    return copies


def fine_scratch():
    both = VMEM((HALVES, FY, FX, LANES), F32)
    return [both] * 3 + [VMEM((FY, FX, LANES), F32)] * 2


def after_kernel(
    u_ref, f_ref, m_ref, e_ref, e_lo, e_hi, n_lo, n_hi, c_lo, c_hi,
    h_el, h_eh, h_nl, h_nh, h_cl, h_ch,
    out_ref, rest_ref,
    us, fs, ms, ws, vs, tmp, sems, out_sems,
):
    copies = fetch((u_ref, f_ref, m_ref), (us, fs, ms), sems)
    strips, old = (e_lo, e_hi, n_lo, n_hi), (h_el, h_eh, h_nl, h_nh)
    outs = []
    for c in range(HALVES):
        h = half(c)
        u, f, m = us.at[c], fs.at[c], ms.at[c]
        mid = pl.ds(LEFT, NX)
        place_lines(u, h, 1, U1, *strips)
        place_lines(u, h, 2, U2, *strips)
        place_corners(u, h, FINE, 0, VALUE_CELLS, c_lo, c_hi)
        for k, dst, slot in ((1, f, F1), (2, m, M1)):
            place_lines(dst, h, 1, slot, *old)
            place_corners(dst, h, FINE, k, FINE_CELLS, h_cl, h_ch)
        for copy in copies[c]:
            copy.wait()

        def add(i, carry):
            for k in range(4):
                line = e_ref[4 * i + k, :, h]
                tmp[k, pl.ds(0, CX, stride=2), :] = line
                tmp[k, pl.ds(1, CX, stride=2), :] = line
            for k in range(4):
                t = tmp[k]
                for j in range(2):
                    r = DEEP + 8 * i + 2 * k + j
                    u[r, mid, :] = u[r, mid, :] + t
            return carry

        lax.fori_loop(0, CY // 4, add, 0)
        two_sweeps(u, vs, f, ws, h, strips, old, mass=m)
        block = (pl.ds(DEEP, NY), mid)
        out = pltpu.make_async_copy(
            u.at[block[0], block[1], :], out_ref.at[:, :, h], out_sems.at[c, 0]
        )
        out.start()
        outs.append(out)

        def rest(i, carry):
            r = DEEP + BLOCK * i
            for k, t, value, s in stencil(u, r, LEFT, NX // 8, BLOCK):
                at = pl.ds(LEFT + 8 * t, 8)
                f[r + k, at, :] = f[r + k, at, :] + s - (4.0 + m[r + k, at, :]) * value
            return carry

        lax.fori_loop(0, NY // BLOCK, rest, 0)
        out = pltpu.make_async_copy(
            f.at[block[0], block[1], :], rest_ref.at[:, :, h], out_sems.at[c, 1]
        )
        out.start()
        outs.append(out)
    for out in outs:
        out.wait()


def after(u, f, m, e, strips, old):
    return pl.pallas_call(
        after_kernel,
        out_shape=(shape(NY, NX, NC),) * 2,
        in_specs=[IN_HBM] * 3 + [IN_VMEM] * 13,
        out_specs=(IN_HBM,) * 2,
        scratch_shapes=fine_scratch()
        + [
            VMEM((4, NX, LANES), F32),
            pltpu.SemaphoreType.DMA((HALVES, 3)),
            pltpu.SemaphoreType.DMA((HALVES, 2)),
        ],
        compiler_params=pltpu.CompilerParams(vmem_limit_bytes=40 * 2**20),
        name="after",
    )(u, f, m, e, *strips, *old)


def body(right_side, first_guess, mass_term):
    f, u, m = right_side, first_guess, mass_term
    nl, nh, knl, knh, tiles = north_edges(u, f, m)
    el, eh, *kept = east_edges(tiles)
    kept += [knl, knh]
    old = halos(FINE_CELLS, NX, el, eh, nl, nh)
    columns = mass_columns(m)
    padded = load(u, f, m)
    mass_strips = exchange(*columns, "east")
    _, _, _, _, u2, right, mass, cel, ceh, cnl, cnh, *u_strips = before(padded, old)
    wide = halos(COARSE_CELLS, CX, cel, ceh, cnl, cnh)
    e, *edge_values = coarse(right, mass, mass_strips, wide, u_strips, kept)
    strips = halos(VALUE_CELLS, NX, *edge_values)
    return after(u2, f, m, e, strips, old)


def solution(mesh):
    spec = P("north", "east", None)
    return jax.shard_map(
        body, mesh=mesh, in_specs=(spec,) * 3, out_specs=(spec, spec), check_vma=False
    )
```
